128 devices in a mesh: group: 8 (over z, x_hi), ep: 16 (over x_lo, y, core).
Axes of the slice: x: 4 (x_hi: 2, x_lo: 2; x = x_hi * 2 + x_lo), y: 4, z: 4, core: 2. Of those that a mesh axis runs over, the one named last changes fastest.
Arguments:
- tokens: bfloat16 [16384, 7168], P(('group', 'ep')), may hold values from -6 to 6
- expert_ids: int32 [16384, 4], P(('group', 'ep')), may hold values from 0 to 63, all different within a row; in each aligned block of 128 rows (0 to 127, 128 to 255, ...) at most 10 rows name the same one
- route_score: float32 [16384, 4], P(('group', 'ep')), may hold values from 0.1 to 1
- gate_weight: bfloat16 [128, 7168, 512], P(('group', 'ep')), may hold values from -0.0625 to 0.0625
- up_weight: bfloat16 [128, 7168, 512], P(('group', 'ep')), may hold values from -0.0625 to 0.0625
- down_weight: bfloat16 [128, 512, 7168], P(('group', 'ep')), may hold values from -0.1875 to 0.1875
Outputs:
- mixed: bfloat16 [16384, 7168], P(('group', 'ep'))
The draws below stay inside these ranges and needn't reach their ends.
Inputs may be any that keep to these rules, and one draw needn't show every extreme that they name: `expert_ids`: among the 128 tokens of one device no expert is named by more than 10 of them, a bound that some block reaches; a token names 4 different experts.
All inputs are finite; a program needn't handle non-finite values.
Results may differ from the reference program's by a relative error of at most 0.0065.
Values may be sent and summed in bfloat16 or wider, within the bound.
A program may use at most 192 MiB of HBM per device.

```python
import math
import jax
import jax.numpy as jnp
import numpy as np
from jax import lax

D = 7168
FF = 1024
FFH = 512
TOPK = 4
TOK_DEV = 128
TOKENS = 16384
EXPERTS = 64
CAP = 10


def levels(key, shape, shards, least, largest):
    gain = 1.0
    for axis_at, shards_of in shards:
        heights = jax.random.uniform(jax.random.fold_in(jax.random.fold_in(key, 6), axis_at), (shards_of,), jnp.float32, least / len(shards), largest / len(shards))
        gain = gain * jnp.repeat(jnp.exp(heights), shape[axis_at] // shards_of).reshape((-1,) + (1,) * (len(shape) - 1 - axis_at))
    return gain


def assign_block(rng, own, number, rows, number_of, top, limit, slope):
    sequence = jax.random.permutation(rng, number_of)
    heavy_load, common = shares(number_of, rows * top, limit, slope, True), shares(number_of, rows * top, limit, slope, False)
    places = jnp.arange(number_of)

    def named(sizes, rotation):
        used = int((sizes > 0).sum())
        fixed = max(1, used // 4)
        shifted = fixed + (places - fixed + rotation * (used - fixed)) % max(1, number_of - fixed)
        return jnp.zeros((number_of,), jnp.int32).at[sequence[jnp.where(places < fixed, places, shifted)]].set(jnp.asarray(sizes, jnp.int32))

    sizes = jnp.where(number % 4 == 0, named(heavy_load, number // 4), named(common, number - number // 4 - 1))
    mixed = jax.random.permutation(jax.random.fold_in(own, 3), number_of)
    giver, receiver = mixed[0:number_of // 2 * 2:2], mixed[1:number_of // 2 * 2:2]
    room = jnp.minimum(sizes[giver] - 1, limit - sizes[receiver]) // 2
    room = jnp.where((giver == sequence[0]) | (receiver == sequence[0]) | (sizes[receiver] == 0), 0, jnp.maximum(room, 0))
    shifted = jax.random.randint(jax.random.fold_in(own, 4), (number_of // 2,), 0, 1 << 20) % (room + 1)
    sizes = sizes.at[giver].add(-shifted).at[receiver].add(shifted)
    items = jnp.searchsorted(jnp.cumsum(sizes), jnp.arange(rows * top), side="right").astype(jnp.int32)
    listing = items.reshape(top, rows).T
    listing = listing[jax.random.permutation(jax.random.fold_in(own, 1), rows)]
    rotation = jax.random.randint(jax.random.fold_in(own, 2), (rows, 1), 0, top)
    return jnp.take_along_axis(listing, (jnp.arange(top)[None, :] + rotation) % top, axis=1)


def shares(number_of, total, most, skew, full):
    portions = [(1 << 20) // math.isqrt(grade ** skew) + 1 for grade in range(1, number_of + 1)]
    largest = most if full else min(most, max(-(-total // number_of), total * portions[0] // sum(portions)))
    least = 1 if total - largest >= number_of - 1 else 0
    given, spare = [largest] + [least] * (number_of - 1), total - largest - least * (number_of - 1)
    while spare > 0:
        free = [i for i in range(1, number_of) if given[i] < largest] or [i for i in range(1, number_of) if given[i] < most]
        whole, remaining = sum([portions[i] for i in free]), spare
        for i in free:
            addition = min(most - given[i], max(1, remaining * portions[i] // whole), spare)
            given[i] = given[i] + addition
            spare = spare - addition
    return np.array(given)


def scatter_about(rng, shape, spread, reach, pieces=(), kind=jnp.bfloat16):
    gain = levels(rng, shape, pieces, -0.22, 0.18) if pieces else 1.0
    values = jax.random.normal(rng, shape, jnp.float32) * spread * gain
    return jnp.minimum(jnp.maximum(values, -reach), reach).astype(kind)


def setup_inputs(seed: int = 0) -> dict:
    keys = jax.random.split(jax.random.key(seed), 7)
    tokens = scatter_about(keys[0], (TOKENS, D), 1.0, 6.0, ((0, 128),))
    expert_ids_keys = jax.random.split(jax.random.fold_in(keys[1], 1), TOKENS // TOK_DEV)
    expert_ids_turns = jax.random.permutation(jax.random.fold_in(keys[1], 3), TOKENS // TOK_DEV)
    expert_ids = jax.vmap(lambda own, number: assign_block(jax.random.fold_in(keys[1], 2), own, number, TOK_DEV, EXPERTS, TOPK, CAP, 2))(expert_ids_keys, expert_ids_turns).reshape((TOKENS, TOPK))
    route_score = jnp.clip(jnp.exp(math.log(1.0) - 2.3025851 * jax.random.uniform(keys[2], (TOKENS, TOPK), jnp.float32) ** levels(keys[2], (TOKENS, TOPK), ((0, 128),), -0.2, 0.2)), 0.1, 1.0)
    gate_weight = scatter_about(keys[3], (2 * EXPERTS, D, FFH), D ** -0.5, 0.0625, ((0, 128),))
    up_weight = scatter_about(keys[4], (2 * EXPERTS, D, FFH), D ** -0.5, 0.0625, ((0, 128),))
    down_weight = scatter_about(keys[5], (2 * EXPERTS, FFH, D), FF ** -0.5, 0.1875, ((0, 128),))
    return {"tokens": tokens, "expert_ids": expert_ids, "route_score": route_score, "gate_weight": gate_weight, "up_weight": up_weight, "down_weight": down_weight}


def reference(tokens, expert_ids, route_score, gate_weight, up_weight, down_weight):
    weight = 2.5 * route_score / jnp.sum(route_score, axis=1, keepdims=True)
    blocks = TOKENS // TOK_DEV
    flat_ids = expert_ids.reshape(blocks, TOK_DEV * TOPK)
    onehot = (flat_ids[:, :, None] == jnp.arange(EXPERTS, dtype=jnp.int32)[None, None, :]).astype(jnp.int32)
    counts = jnp.cumsum(onehot, axis=1)
    slot_of = jnp.sum(onehot * counts, axis=2) - 1
    position = jnp.arange(blocks, dtype=jnp.int32)[:, None] * CAP + slot_of
    token_flat = jnp.arange(TOKENS * TOPK, dtype=jnp.int32) // TOPK
    table_tok = jnp.zeros((EXPERTS, blocks * CAP), jnp.int32).at[flat_ids.reshape(-1), position.reshape(-1)].set(token_flat)
    table_wt = jnp.zeros((EXPERTS, blocks * CAP), jnp.float32).at[flat_ids.reshape(-1), position.reshape(-1)].set(weight.reshape(-1))

    def add_expert(running, entry):
        expert, rows_tok, rows_wt = entry
        gathered = tokens[rows_tok]
        combined = jnp.zeros((rows_tok.shape[0], D), jnp.float32)
        for which_half in range(2):
            w_index = expert * 2 + which_half
            gate_rows = lax.dynamic_index_in_dim(gate_weight, w_index, 0, keepdims=False)
            up_rows = lax.dynamic_index_in_dim(up_weight, w_index, 0, keepdims=False)
            down_rows = lax.dynamic_index_in_dim(down_weight, w_index, 0, keepdims=False)
            gate_out = jnp.dot(gathered, gate_rows, preferred_element_type=jnp.float32)
            up_out = jnp.dot(gathered, up_rows, preferred_element_type=jnp.float32)
            hidden = (jax.nn.silu(gate_out) * up_out).astype(jnp.bfloat16)
            part = jnp.dot(hidden, down_rows, preferred_element_type=jnp.float32).astype(jnp.bfloat16)
            combined = combined + part.astype(jnp.float32)
        expert_out = combined.astype(jnp.bfloat16).astype(jnp.float32)
        running = running.at[rows_tok].add(rows_wt[:, None] * expert_out)
        return running, None

    running, _ = lax.scan(add_expert, jnp.zeros((TOKENS, D), jnp.float32),
                          (jnp.arange(EXPERTS, dtype=jnp.int32), table_tok, table_wt))
    return running.astype(jnp.bfloat16)
```

```python
import functools

import jax
import jax.numpy as jnp
from jax import lax
from jax.experimental import pallas as pl
from jax.experimental.pallas import tpu as pltpu
from jax.sharding import PartitionSpec as P

D = 7168
FFH = 512
TOPK = 4
TOK = 128
EXPERTS = 64
HEAD = 8
QUARTER = D // 4
CHUNKS = 4
PER = EXPERTS // CHUNKS
ROWS = PER * HEAD + PER * 2
MESH = pl.DeviceIdType.MESH
F32 = jnp.float32
BF16 = jnp.bfloat16


def iota(shape, dim):
    return lax.broadcasted_iota(jnp.int32, shape, dim)


def prep_kernel(tokens, ids, score, head, tail, w_head, w_tail):
    weight = 2.5 * score[...] / jnp.sum(score[...], axis=1, keepdims=True)
    expert = iota((TOK, EXPERTS), 1)
    named = [(ids[:, k : k + 1] == expert).astype(F32) for k in range(TOPK)]
    before = (iota((TOK, TOK), 1) < iota((TOK, TOK), 0)).astype(BF16)
    counts = jnp.dot(before, sum(named).astype(BF16), preferred_element_type=F32)
    column = iota((TOK, EXPERTS * HEAD), 1)
    pick_head = jnp.zeros((TOK, EXPERTS * HEAD), F32)
    pick_tail = jnp.zeros((TOK, EXPERTS * HEAD), F32)
    wt_head = jnp.zeros((TOK, EXPERTS * HEAD), F32)
    wt_tail = jnp.zeros((TOK, EXPERTS * HEAD), F32)
    for k in range(TOPK):
        slot = jnp.sum(counts * named[k], axis=1, keepdims=True).astype(jnp.int32)
        own = (column // HEAD) == ids[:, k : k + 1]
        hit_head = jnp.where(own & (column % HEAD == slot), 1.0, 0.0)
        hit_tail = jnp.where(own & (column % 2 + HEAD == slot), 1.0, 0.0)
        pick_head += hit_head
        pick_tail += hit_tail
        wt_head += hit_head * weight[:, k : k + 1]
        wt_tail += hit_tail * weight[:, k : k + 1]
    w_head[...] = wt_head.astype(BF16)
    w_tail[...] = wt_tail.astype(BF16)
    contract = (((0,), (0,)), ((), ()))
    rows = pick_head.T.astype(BF16)
    for n in range(4):
        at = slice(n * QUARTER, (n + 1) * QUARTER)
        head[:, at] = jnp.dot(rows, tokens[:, at], preferred_element_type=F32).astype(BF16)
    turned = pick_tail.T
    quarter = (iota((EXPERTS * HEAD, TOK), 0) % HEAD) // 2
    total = jnp.zeros((EXPERTS * HEAD, QUARTER), F32)
    for q in range(4):
        part = jnp.where(quarter == q, turned, 0.0).astype(BF16)
        at = slice(q * QUARTER, (q + 1) * QUARTER)
        total += jnp.dot(part, tokens[:, at], preferred_element_type=F32)
    tail[...] = total.astype(BF16)


def prep(tokens, ids, score):
    wide = EXPERTS * HEAD
    return pl.pallas_call(
        prep_kernel,
        out_shape=(
            jax.ShapeDtypeStruct((wide, D), BF16),
            jax.ShapeDtypeStruct((wide, QUARTER), BF16),
            jax.ShapeDtypeStruct((TOK, wide), BF16),
            jax.ShapeDtypeStruct((TOK, wide), BF16),
        ),
        compiler_params=pltpu.CompilerParams(vmem_limit_bytes=48 * 2**20),
    )(tokens, ids, score)


def offset(i):
    i0, i1, i2 = i % 4, (i // 4) % 4, i // 16
    return i0, (i0 + i1) % 4, (i0 + i1 + i2) % 4


def device(z, x, y, c):
    return (z * 2 + x // 2, ((x % 2) * 4 + y) * 2 + c)


def moe_kernel(
    head, tail, wg, wu, wd, yh, yt,
    xs, ts, wgv, wuv, wdv, hid,
    own_sem, give_sem, take_sem,
    out_h, out_t, in_h, in_t, ret_h, ret_t, back_h, back_t,
):
    group, ep = lax.axis_index("group"), lax.axis_index("ep")
    z, x, y, c = group // 2, (group % 2) * 2 + ep // 8, (ep // 2) % 4, ep % 2
    me = z * 16 + x * 4 + y

    def ahead(i):
        dz, dx, dy = offset(i)
        tz, tx, ty = (z + dz) % 4, (x + dx) % 4, (y + dy) % 4
        return tz * 16 + tx * 4 + ty, device(tz, tx, ty, c)

    def behind(i):
        dz, dx, dy = offset(i)
        return device((z + 4 - dz) % 4, (x + 4 - dx) % 4, (y + 4 - dy) % 4, c)

    def block(i):
        return pl.ds(pl.multiple_of(i * HEAD, HEAD), HEAD)

    barrier = pltpu.get_barrier_semaphore()

    def greet(i, carry):
        pl.semaphore_signal(barrier, inc=1, device_id=ahead(i)[1], device_id_type=MESH)
        return carry

    lax.fori_loop(1, EXPERTS, greet, 0)
    partner = device(z, x, y, 1 - c)
    pl.semaphore_signal(barrier, inc=1, device_id=partner, device_id_type=MESH)
    pl.semaphore_wait(barrier, EXPERTS)

    pltpu.make_async_copy(head.at[block(me)], xs.at[0, block(0)], in_h.at[0]).start()
    pltpu.make_async_copy(tail.at[block(me)], ts.at[0, block(0)], in_t.at[0]).start()

    def dispatch(i, carry):
        chip, dev = ahead(i)
        pltpu.make_async_remote_copy(
            src_ref=head.at[block(chip)], dst_ref=xs.at[i // PER, block(i % PER)],
            send_sem=out_h, recv_sem=in_h.at[i // PER], device_id=dev, device_id_type=MESH,
        ).start()
        pltpu.make_async_remote_copy(
            src_ref=tail.at[block(chip)], dst_ref=ts.at[i // PER, block(i % PER)],
            send_sem=out_t, recv_sem=in_t.at[i // PER], device_id=dev, device_id_type=MESH,
        ).start()
        return carry

    lax.fori_loop(1, EXPERTS, dispatch, 0)

    own, give = [], []
    for n, (source, target) in enumerate(((wg, wgv), (wu, wuv), (wd, wdv))):
        own.append(pltpu.make_async_copy(source.at[0], target.at[0], own_sem.at[n]))
        give.append(pltpu.make_async_remote_copy(
            src_ref=source.at[0], dst_ref=target.at[1],
            send_sem=give_sem.at[n], recv_sem=take_sem.at[n],
            device_id=partner, device_id_type=MESH,
        ))
        own[-1].start()
        give[-1].start()

    a = iota((PER * HEAD, PER * HEAD), 0)
    b = iota((PER * HEAD, PER * HEAD), 1)
    spread = (b == (a % 32) // 2 * HEAD + a // 32 * 2 + a % 2).astype(BF16)
    gather = (a == (b % 32) // 2 * HEAD + b // 32 * 2 + b % 2).astype(BF16)
    top = PER * HEAD

    def step(chunk, carry):
        pltpu.make_async_copy(
            xs.at[chunk, pl.ds(0, top)], xs.at[chunk, pl.ds(0, top)], in_h.at[chunk]
        ).wait()
        pltpu.make_async_copy(ts.at[chunk], ts.at[chunk], in_t.at[chunk]).wait()

        @pl.when(chunk == 0)
        def _():
            for n in range(3):
                own[n].wait()
                give[n].wait_recv()

        moved = jnp.dot(spread, ts[chunk], preferred_element_type=F32).astype(BF16)
        for q in range(4):
            xs[chunk, top:, q * QUARTER : (q + 1) * QUARTER] = moved[q * 32 : (q + 1) * 32]

        def up(n, carry):
            at = pl.ds(pl.multiple_of((n % 2) * 256, 256), 256)
            gate = jnp.zeros((ROWS, 256), F32)
            lift = jnp.zeros((ROWS, 256), F32)
            for k in range(7):
                rows = slice(k * 1024, (k + 1) * 1024)
                left = xs[chunk, :, rows]
                gate += jnp.dot(left, wgv[n // 2, rows, at], preferred_element_type=F32)
                lift += jnp.dot(left, wuv[n // 2, rows, at], preferred_element_type=F32)
            hid[n] = (gate / (1.0 + jnp.exp(-gate)) * lift).astype(BF16)
            return carry

        lax.fori_loop(0, 4, up, 0)

        def down(n, carry):
            at = pl.ds(pl.multiple_of(n * 512, 512), 512)
            total = jnp.zeros((ROWS, 512), F32)
            for k in range(4):
                total += jnp.dot(
                    hid[k], wdv[k // 2, (k % 2) * 256 : (k % 2) * 256 + 256, at],
                    preferred_element_type=F32,
                )
            xs[chunk, :, at] = total.astype(BF16)
            return carry

        lax.fori_loop(0, 14, down, 0)

        stacked = jnp.concatenate(
            [xs[chunk, top:, q * QUARTER : (q + 1) * QUARTER] for q in range(4)], axis=0
        )
        ts[chunk] = jnp.dot(gather, stacked, preferred_element_type=F32).astype(BF16)

        def back(r, carry):
            i = chunk * PER + r

            @pl.when(i == 0)
            def _():
                pltpu.make_async_copy(xs.at[0, block(0)], yh.at[block(me)], back_h).start()
                pltpu.make_async_copy(ts.at[0, block(0)], yt.at[block(me)], back_t).start()

            @pl.when(i > 0)
            def _():
                dev = behind(i)
                pltpu.make_async_remote_copy(
                    src_ref=xs.at[chunk, block(r)], dst_ref=yh.at[block(me)],
                    send_sem=ret_h, recv_sem=back_h, device_id=dev, device_id_type=MESH,
                ).start()
                pltpu.make_async_remote_copy(
                    src_ref=ts.at[chunk, block(r)], dst_ref=yt.at[block(me)],
                    send_sem=ret_t, recv_sem=back_t, device_id=dev, device_id_type=MESH,
                ).start()

            return carry

        lax.fori_loop(0, PER, back, 0)
        return carry

    lax.fori_loop(0, CHUNKS, step, 0)
    for n in range(3):
        give[n].wait_send()
    most = pl.ds(0, (EXPERTS - 1) * HEAD)
    for sem, ref in ((out_h, yh.at[most]), (out_t, yt.at[most]), (ret_h, yh.at[most]),
                     (ret_t, yt.at[most]), (back_h, yh), (back_t, yt)):
        pltpu.make_async_copy(ref, ref, sem).wait()


def moe(head, tail, wg, wu, wd):
    anywhere = pl.BlockSpec(memory_space=pltpu.HBM)
    dma = pltpu.SemaphoreType.DMA
    return pl.pallas_call(
        moe_kernel,
        out_shape=(
            jax.ShapeDtypeStruct((EXPERTS * HEAD, D), BF16),
            jax.ShapeDtypeStruct((EXPERTS * HEAD, QUARTER), BF16),
        ),
        in_specs=[anywhere] * 5,
        out_specs=(anywhere, anywhere),
        scratch_shapes=[
            pltpu.VMEM((CHUNKS, ROWS, D), BF16),
            pltpu.VMEM((CHUNKS, PER * HEAD, QUARTER), BF16),
            pltpu.VMEM((2, D, FFH), BF16),
            pltpu.VMEM((2, D, FFH), BF16),
            pltpu.VMEM((2, FFH, D), BF16),
            pltpu.VMEM((4, ROWS, 256), BF16),
            dma((3,)), dma((3,)), dma((3,)),
            dma, dma, dma((CHUNKS,)), dma((CHUNKS,)), dma, dma, dma, dma,
        ],
        compiler_params=pltpu.CompilerParams(
            collective_id=0, has_side_effects=True, vmem_limit_bytes=67043328
        ),
    )(head, tail, wg, wu, wd)


def combine_kernel(w_head, w_tail, yh, yt, out):
    quarter = (iota((TOK, EXPERTS * HEAD), 1) % HEAD) // 2
    mine = jnp.where(quarter == pl.program_id(0), w_tail[...].astype(F32), 0.0).astype(BF16)
    total = jnp.dot(w_head[...], yh[...], preferred_element_type=F32)
    total += jnp.dot(mine, yt[...], preferred_element_type=F32)
    out[...] = total.astype(BF16)


def combine(w_head, w_tail, yh, yt):
    wide = EXPERTS * HEAD
    return pl.pallas_call(
        combine_kernel,
        grid=(4,),
        out_shape=jax.ShapeDtypeStruct((TOK, D), BF16),
        in_specs=[
            pl.BlockSpec((TOK, wide), lambda q: (0, 0)),
            pl.BlockSpec((TOK, wide), lambda q: (0, 0)),
            pl.BlockSpec((wide, QUARTER), lambda q: (0, q)),
            pl.BlockSpec((wide, QUARTER), lambda q: (0, 0)),
        ],
        out_specs=pl.BlockSpec((TOK, QUARTER), lambda q: (0, q)),
        compiler_params=pltpu.CompilerParams(vmem_limit_bytes=32 * 2**20),
    )(w_head, w_tail, yh, yt)


def shards(tokens, expert_ids, route_score, gate_weight, up_weight, down_weight):
    head, tail, w_head, w_tail = prep(tokens, expert_ids, route_score)
    yh, yt = moe(head, tail, gate_weight, up_weight, down_weight)
    return combine(w_head, w_tail, yh, yt)


def solution(mesh):
    tokens = P(("group", "ep"), None)
    weights = P(("group", "ep"), None, None)
    return jax.shard_map(
        shards, mesh=mesh, in_specs=(tokens,) * 3 + (weights,) * 3, out_specs=tokens,
        check_vma=False,
    )
```
